32 devices in a mesh: row: 4 (over x, core), col: 8 (over z, y).
Axes of the slice: x: 2, y: 2, z: 4, core: 2. Of those that a mesh axis runs over, the one named last changes fastest.
Arguments:
- matrix: float32 [16, 4, 256, 8, 8, 256], P(None, 'row', None, None, 'col'), may hold values from -3 to 8
Outputs:
- factored: float32 [16, 4, 256, 8, 8, 256], P(None, 'row', None, None, 'col')
The draws below stay inside these ranges and needn't reach their ends.
All inputs are finite; a program needn't handle non-finite values.
Results may differ from the reference program's by a relative error of at most 0.0001.
Values sent between devices are 32-bit elements; how exact they have to be, the bound alone decides.
No kernel may reach another device: no remote copies, remote signals or barrier semaphores. Data moves between devices by JAX's collectives and lax.ppermute only.
A program may use at most 192 MiB of HBM per device.

```python
import jax
import jax.numpy as jnp
from jax import lax

ORDER = 16384
NB = 256
SEGMENTS = 3
BLOCKS = 64
N_ROW = 4
N_COL = 8


def draw_matrix(key, part):
    first, second, third = jax.random.split(jax.random.fold_in(key, 11), 3)
    width = 2 * NB
    noise_scale = 0.8 / (2.0 * ORDER) ** 0.5
    factors = jax.random.normal(first, (ORDER, width), jnp.float32)
    diagonal = 2.0 + jnp.exp(jax.random.uniform(second, (ORDER,), jnp.float32, jnp.log(0.5), jnp.log(2.0)))
    rough = jax.random.truncated_normal(third, -4.0, 4.0, (ORDER, ORDER), jnp.float32)
    gram = jnp.dot(factors, factors.T, precision=lax.Precision.HIGHEST) / width
    whole = 0.5 * (gram + gram.T) + noise_scale * (rough + rough.T)
    positions = jnp.arange(ORDER, dtype=jnp.int32)
    whole = whole.at[positions, positions].add(diagonal)
    return whole.reshape(BLOCKS // N_ROW, N_ROW, NB, BLOCKS // N_COL, N_COL, NB)


def setup_inputs(seed: int = 0) -> dict:
    arg_keys = jax.random.split(jax.random.key(seed), 2)
    return {
        "matrix": draw_matrix(jax.random.fold_in(arg_keys[1], 71), 0),
    }


def reference(matrix):
    whole = matrix.reshape(ORDER, ORDER)
    identity = jnp.eye(NB, dtype=whole.dtype)
    for segment in range(SEGMENTS):
        start = segment * NB
        diagonal = whole[start:start + NB, start:start + NB]
        lower = jnp.linalg.cholesky(diagonal)
        inverse = lax.linalg.triangular_solve(lower, identity, left_side=True, lower=True)
        column = whole[start:, start:start + NB]
        panel = jnp.dot(column, inverse.T, precision=lax.Precision.HIGHEST)
        whole = whole.at[start:, start:start + NB].set(panel)
        below = panel[NB:]
        trailing = whole[start + NB:, start + NB:] - jnp.dot(below, below.T, precision=lax.Precision.HIGHEST)
        whole = whole.at[start + NB:, start + NB:].set(trailing)
    return whole.reshape(matrix.shape)
```

```python
import functools

import jax
import jax.numpy as jnp
from jax import lax
from jax.experimental import pallas as pl
from jax.experimental.pallas import tpu as pltpu
from jax.sharding import PartitionSpec as P

SEGMENTS = 3
TILE = 128
CHUNKS = 2
HIGHEST = lax.Precision.HIGHEST


def eliminate(block):
    rows = lax.broadcasted_iota(jnp.int32, (TILE, TILE), 0)
    lanes = lax.broadcasted_iota(jnp.int32, (TILE, TILE), 1)
    group = 8
    parts = [block[i : i + group, :] for i in range(0, TILE, group)]
    lane = lax.broadcasted_iota(jnp.int32, (group, TILE), 1)
    sub = lax.broadcasted_iota(jnp.int32, (group, TILE), 0)
    for k in range(TILE):
        g = k // group
        column = [jnp.broadcast_to(part[:, k : k + 1], (group, TILE)) for part in parts[g:]]
        here = k % group
        pivot = column[0][here : here + 1, :]
        row = parts[g][here : here + 1, :]
        scaled = jnp.where(lane[:1] == k, 1.0, row) / pivot
        scaled = jnp.broadcast_to(scaled, (group, TILE))
        for i in range(g, TILE // group):
            kept = jnp.where(lane == k, 0.0, parts[i])
            new = kept - column[i - g] * scaled
            if i == g:
                new = jnp.where(sub > here, new, parts[i])
            parts[i] = new
    done = jnp.concatenate(parts, axis=0)
    diagonal = jnp.sum(jnp.where(rows == lanes, done, 0.0), axis=1, keepdims=True)
    unit = jnp.where(rows == lanes, 1.0, jnp.where(rows > lanes, done, 0.0))
    return unit * lax.rsqrt(diagonal)


def cut(value):
    high = value.astype(jnp.bfloat16)
    return high, (value - high.astype(jnp.float32)).astype(jnp.bfloat16)


def split(value):
    rounded = lax.reduce_precision(value, exponent_bits=8, mantissa_bits=7)
    return rounded.astype(jnp.bfloat16), (value - rounded).astype(jnp.bfloat16)


def product(left, right):
    total = jnp.dot(left[0], right[0], preferred_element_type=jnp.float32)
    total += jnp.dot(left[1], right[0], preferred_element_type=jnp.float32)
    return total + jnp.dot(left[0], right[1], preferred_element_type=jnp.float32)


def exact(left, right, contract=((1,), (0,))):
    return lax.dot_general(
        left, right, (contract, ((), ())), precision=HIGHEST, preferred_element_type=jnp.float32
    )


def segment_kernel(panel, start, column, *refs):
    out, work, inverse = refs[-3:]
    work[...] = column[start:, :]
    if start:
        before = refs[0]
        cross = exact(before[...], column[:start, :])
        work[...] = work[...] - exact(cross, cross, ((0,), (0,)))
    blocks = panel // TILE

    def step(b, carry):
        at = pl.ds(pl.multiple_of(b * TILE, TILE), TILE)
        corner = eliminate(work[at, at])
        strip = exact(corner, work[at, :])
        place = lax.broadcasted_iota(jnp.int32, strip.shape, 1) // TILE
        strip = jnp.where(place == b, jnp.concatenate([corner] * blocks, axis=1), strip)
        inverse[at, :] = jnp.where(place <= b, strip, 0.0)
        factor = jnp.where(place > b, strip, 0.0)
        below = lax.broadcasted_iota(jnp.int32, (panel, TILE), 0) // TILE > b
        work[:, at] = jnp.where(below, 0.0, work[:, at])
        work[...] = work[...] - exact(factor, strip, ((0,), (0,)))
        return carry

    lax.fori_loop(0, blocks, step, 0)
    out[start:, start:] = inverse[...]
    if start:
        out[:start, :start] = before[...]
        out[:start, start:] = jnp.zeros((start, panel), jnp.float32)
        out[start:, :start] = -exact(inverse[...], exact(cross, before[...], ((0,), (0,))))


def segment_inverse(column, before, panel):
    order = column.shape[0]
    operands = (column,) if before is None else (column, before)
    return pl.pallas_call(
        functools.partial(segment_kernel, panel, order - panel),
        out_shape=jax.ShapeDtypeStruct((order, order), jnp.float32),
        in_specs=[pl.BlockSpec(memory_space=pltpu.VMEM)] * len(operands),
        out_specs=pl.BlockSpec(memory_space=pltpu.VMEM),
        scratch_shapes=[pltpu.VMEM((panel, panel), jnp.float32)] * 2,
        compiler_params=pltpu.CompilerParams(vmem_limit_bytes=40 * 2**20),
        cost_estimate=pl.CostEstimate(
            flops=2 * 10**10, bytes_accessed=8 * order * order, transcendentals=0
        ),
        name="segment_inverse",
    )(*operands)


def columns_kernel(panel, segments, index, inv_high, inv_low, value, high, low):
    q = pl.program_id(0)
    global_col = q * index[0] + index[1]
    right = cut(value[0])
    for s in range(segments):
        deep, rows = (s + 1) * panel, slice(s * panel, (s + 1) * panel)
        part = product(
            (inv_high[rows, :deep], inv_low[rows, :deep]), (right[0][:deep, :], right[1][:deep, :])
        )
        part = jnp.where(global_col > s, part, 0.0)
        high[rows, :], low[rows, :] = cut(part)


def column_panels(whole, index, inverse, panel):
    count, depth, _ = whole.shape
    shape = jax.ShapeDtypeStruct((depth, count * panel), jnp.bfloat16)
    full = pl.BlockSpec((depth, depth), lambda q, index: (0, 0))
    spot = pl.BlockSpec((depth, panel), lambda q, index: (0, q))
    return pl.pallas_call(
        functools.partial(columns_kernel, panel, depth // panel),
        grid_spec=pltpu.PrefetchScalarGridSpec(
            num_scalar_prefetch=1,
            grid=(count,),
            in_specs=[full, full, pl.BlockSpec((1, depth, panel), lambda q, index: (q, 0, 0))],
            out_specs=[spot, spot],
        ),
        out_shape=(shape, shape),
        compiler_params=pltpu.CompilerParams(
            vmem_limit_bytes=40 * 2**20, dimension_semantics=("arbitrary",)
        ),
        cost_estimate=pl.CostEstimate(
            flops=6 * depth * depth * count * panel, bytes_accessed=8 * depth * count * panel, transcendentals=0
        ),
        name="column_panels",
    )(index, *inverse, whole)


def update_kernel(panel, segments, row_step, index, near, far, inv_high, inv_low, *refs):
    col_high, col_low, matrix = refs[:3]
    out, kept = refs[-2:]
    my_row, my_col = index[1], index[2]
    place = index[3] + pl.program_id(0) * index[4]
    global_row = place * row_step + my_row
    pieces = matrix.shape[0] // panel
    value = cut(jnp.where(index[0] == 1, near[0], far[0]).T)
    highs, lows = [], []
    for s in range(segments):
        deep, lanes = (s + 1) * panel, slice(s * panel, (s + 1) * panel)
        part = product(
            (value[0][:, :deep], value[1][:, :deep]), (inv_high[:deep, lanes], inv_low[:deep, lanes])
        )
        kept[:, lanes] = part
        high, low = cut(jnp.where(global_row > s, part, 0.0))
        highs.append(high)
        lows.append(low)
    left = (jnp.concatenate(highs, axis=1), jnp.concatenate(lows, axis=1))
    for c in range(0, pieces * TILE, panel):
        change = product(left, (col_high[:, c : c + panel], col_low[:, c : c + panel]))
        for t in range(0, panel, TILE):
            at = pl.ds((c + t) // TILE, panel, stride=pieces)
            out[at, :] = matrix[at, :] - change[:, t : t + TILE]

    for s in range(segments):

        @pl.when(jnp.logical_and(my_col == s, global_row >= s))
        def _():
            for t in range(0, panel, TILE):
                at = pl.ds(t // TILE, panel, stride=pieces)
                out[at, :] = kept[:, s * panel + t : s * panel + t + TILE]


def update(flat, previous, index, near, far, inverse, columns, panel, row_step):
    count, depth, _ = near.shape
    width = columns[0].shape[1]
    rows_flat = panel * width // TILE

    def at_place(g, index):
        return (index[3] + g * index[4], 0)

    block = pl.BlockSpec((1, depth, panel), lambda g, index: (g, 0, 0))
    square = pl.BlockSpec((depth, depth), lambda g, index: (0, 0))
    wide = pl.BlockSpec((depth, width), lambda g, index: (0, 0))
    in_specs = [block, block, square, square, wide, wide, pl.BlockSpec((rows_flat, TILE), at_place)]
    operands = [near, far, *inverse, *columns, flat]
    aliases = {}
    if previous is not None:
        in_specs.append(pl.BlockSpec(memory_space=pl.ANY))
        operands.append(previous)
        aliases = {len(operands): 0}
    return pl.pallas_call(
        functools.partial(update_kernel, panel, SEGMENTS, row_step),
        grid_spec=pltpu.PrefetchScalarGridSpec(
            num_scalar_prefetch=1,
            grid=(count,),
            in_specs=in_specs,
            out_specs=pl.BlockSpec((rows_flat, TILE), at_place),
            scratch_shapes=[pltpu.VMEM((panel, depth), jnp.float32)],
        ),
        out_shape=jax.ShapeDtypeStruct(flat.shape, jnp.float32),
        input_output_aliases=aliases,
        compiler_params=pltpu.CompilerParams(
            vmem_limit_bytes=52 * 2**20, dimension_semantics=("arbitrary",)
        ),
        cost_estimate=pl.CostEstimate(
            flops=6 * count * panel * depth * (width + depth),
            bytes_accessed=8 * count * panel * width,
            transcendentals=0,
        ),
        name="panel_update",
    )(index, *operands)


def over_rows(value, row_count):
    held = {0: value}
    bit = row_count // 2
    while bit:
        pairs = [(r, r ^ bit) for r in range(row_count)]
        held.update({d | bit: lax.ppermute(v, "row", pairs) for d, v in list(held.items())})
        bit //= 2
    my_row = lax.axis_index("row")
    picked = []
    for k in range(SEGMENTS):
        distance = jnp.bitwise_xor(my_row, k)
        chosen = held[0]
        for d in range(1, row_count):
            chosen = jnp.where(distance == d, held[d], chosen)
        picked.append(chosen)
    return jnp.concatenate(picked, axis=1)


def spread(value, root, col_count):
    mine = lax.axis_index("col") == root
    value = jnp.where(mine, value, 0.0)
    have = [root]
    bit = col_count // 2
    while bit:
        value = value + lax.ppermute(value, "col", [(s, s ^ bit) for s in have])
        have += [s ^ bit for s in have]
        bit //= 2
    return value


class Exchange:
    def __init__(self, row_count, col_count):
        self.rows, self.cols, self.layers = row_count, col_count, col_count // 2
        self.half = row_count // 2
        my_row, my_col = lax.axis_index("row"), lax.axis_index("col")
        my_z = my_col // 2
        self.depth = jnp.where(my_row < self.half, my_z, self.layers - 1 - my_z)
        self.home = (my_col % 2 == my_row % 2).astype(jnp.int32)
        flip = jnp.bitwise_xor((my_row >= self.half).astype(jnp.int32), (self.depth >= 2).astype(jnp.int32))
        self.classes = (flip, 1 - flip)

    def device(self, r, depth, y):
        z = depth if r < self.half else self.layers - 1 - depth
        return r * self.cols + z * 2 + y

    def move(self, value, steps, across=False):
        pairs = []
        for r in range(self.rows):
            y = r % 2
            for a, b in steps:
                pairs.append((self.device(r, a, y), self.device(r, b, 1 - y if across else y)))
        return lax.ppermute(value, ("row", "col"), pairs)

    def cross(self, value):
        return self.move(value, [(d, d) for d in range(self.layers)], across=True)

    def one(self, own):
        return self.move(own, [(0, 1), (2, 3)]), self.move(own, [(2, 1)])

    def two(self, own, up, down):
        first = jnp.where(self.depth % 2 == 0, own, up)
        return self.move(up, [(1, 2)]), self.move(down, [(1, 0)]), first, self.cross(first)

    def three(self, down, up_again, down_again):
        up_last = self.move(up_again, [(2, 3)])
        second = jnp.where(self.depth == 1, down, jnp.where(self.depth == 2, up_again, up_last))
        second = jnp.where(self.depth == 0, down_again, second)
        return second, self.cross(second)


def after(values, token):
    return lax.optimization_barrier((*values, token))[:-1]


def gathered(own, row_count, col_count):
    everything = lax.all_gather(own, "col")
    my_row = lax.axis_index("row")
    items = []
    for c in range(0, col_count, row_count):
        value = lax.dynamic_index_in_dim(everything, my_row + c, 0, keepdims=False)
        items.append((value, value, jnp.int32(c // row_count)))
    return items


def local(matrix):
    row_blocks, _, panel, col_blocks, _, _ = matrix.shape
    row_count = lax.axis_size("row")
    col_count = lax.axis_size("col")
    classes = col_count // row_count
    my_row, my_col = lax.axis_index("row"), lax.axis_index("col")
    flat = matrix.reshape(row_blocks * panel * col_blocks * panel // TILE, TILE)
    raw = jnp.transpose(matrix[0, 0, :, :, 0, :], (1, 0, 2))
    chunk = max(1, col_blocks // CHUNKS)
    lead = over_rows(raw[:1], row_count)
    ahead = [spread(lead[0, : (k + 1) * panel], k, col_count) for k in range(SEGMENTS)]
    starts = list(range(0, col_blocks, chunk))
    held = []
    for q in starts:
        low = max(q, 1)
        parts = [lead] if q == 0 else []
        if q + chunk > low:
            parts.append(over_rows(raw[low : q + chunk], row_count))
        held.append(jnp.concatenate(parts, axis=0))

    fast = row_count == 4 and classes == 2
    inverse = None
    if fast:
        plan = Exchange(row_count, col_count)
        state = [{} for _ in starts]
        for stage in range(SEGMENTS):
            ready = min(stage + 1, len(starts))
            for n in range(ready):
                own = held[n]
                if stage == n:
                    state[n]["one"] = plan.one(own if inverse is None else after((own,), inverse)[0])
                if stage == n + 1:
                    up, down = after(state[n]["one"], inverse)
                    state[n]["two"] = plan.two(own, up, down)
                if stage == n + 2:
                    values = after((state[n]["one"][1], *state[n]["two"][:2]), inverse)
                    state[n]["three"] = plan.three(*values)
            inverse = segment_inverse(ahead[stage], inverse, panel)
        for n, own in enumerate(held):
            now = state[n]
            if "one" not in now:
                now["one"] = plan.one(own)
            if "two" not in now:
                now["two"] = plan.two(own, *now["one"])
            if "three" not in now:
                now["three"] = plan.three(now["one"][1], *now["two"][:2])
    else:
        for k in range(SEGMENTS):
            inverse = segment_inverse(ahead[k], inverse, panel)

    whole = jnp.concatenate(held, axis=0)
    place = jnp.stack([jnp.int32(col_count), my_col]).astype(jnp.int32)
    columns = column_panels(whole, place, split(inverse), panel)
    turned = split(inverse.T)
    out = None
    for n, q in enumerate(starts):
        if fast:
            _, _, first, first_far = state[n]["two"]
            second, second_far = state[n]["three"]
            items = [(first, first_far, plan.classes[0]), (second, second_far, plan.classes[1])]
            home = plan.home
        else:
            items, home = gathered(held[n], row_count, col_count), jnp.int32(1)
        for near, far, which in items:
            index = jnp.stack([home, my_row, my_col, q * classes + which, jnp.int32(classes)])
            out = update(flat, out, index.astype(jnp.int32), near, far, turned, columns, panel, row_count)
    return out.reshape(matrix.shape)


def solution(mesh):
    spec = P(None, "row", None, None, "col", None)
    return jax.shard_map(local, mesh=mesh, in_specs=(spec,), out_specs=spec, check_vma=False)
```
